256 devices in a mesh: section: 2 (over core), rep: 16 (over z_lo, y), tp: 8 (over z_hi, x).
Axes of the slice: x: 4, y: 4, z: 8 (z_hi: 2, z_lo: 4; z = z_hi * 4 + z_lo), core: 2. Of those that a mesh axis runs over, the one named last changes fastest.
Arguments:
- tokens: bfloat16 [32768, 8192], P(('section', 'rep'), 'tp'), may hold values from -6 to 6
- norm_gain: bfloat16 [8192], P('tp'), may hold values from 0.099609375 to 1.8984375
- kv_weight: bfloat16 [8192, 2048], P('tp'), may hold values from -0.0625 to 0.0625
- page_dest: int32 [2048, 1], P(('section', 'rep')), may hold values from 0 to 31; in each aligned block of 64 rows (0 to 63, 64 to 127, ...) at most 4 rows name the same one
- page_row: int32 [2048], P(('section', 'rep')), may hold values from 0 to 7
- queries: bfloat16 [256, 8192], P(('section', 'rep'), 'tp'), may hold values from -250 to 250
- kv_pool: bfloat16 [1024, 16, 2048], P(('section', 'rep'), None, 'tp'), may hold values from -9 to 9
- block_table: int32 [256, 4], P(('section', 'rep')), may hold values from 0 to 31, as said below
- ctx_len: int32 [256], P(('section', 'rep')), may hold values from 2 to 64
- new_kv: bfloat16 [256, 2048], P(('section', 'rep'), 'tp'), may hold values from -6 to 6
Outputs:
- attended: bfloat16 [256, 8192], P(('section', 'rep'), 'tp')
The draws below stay inside these ranges and needn't reach their ends.
Inputs may be any that keep to these rules, and one draw needn't show every extreme that they name: `page_dest`: at most 4 of the new pages of one owner go to the same owner. `block_table`: the rows of one owner name each of its 32 local pages exactly once.
All inputs are finite; a program needn't handle non-finite values.
Results may differ from the reference program's by a relative error of at most 0.019.
Values may be sent and summed in bfloat16 or wider, within the bound.
No kernel may reach another device: no remote copies, remote signals or barrier semaphores. Data moves between devices by JAX's collectives and lax.ppermute only.
A program may use at most 64 MiB of HBM per device.

```python
import math
import jax
import jax.numpy as jnp
import numpy as np
from jax import lax

D = 8192
H = 64
KV = 8
HD = 128
PAGE = 16
MAXP = 4
ROWS_DEV = 8
OWNERS = 32
TOKENS = 32768
PAGES_DEV = 64
NEWPAGES = 2048
SLOT = 4
ROWS_TOTAL = 256
RES_PAGES = 32
N_TP = 8


def page_table(key):
    keys = jax.random.split(jax.random.fold_in(key, 11), OWNERS)
    perms = jax.vmap(lambda k: jax.random.permutation(k, RES_PAGES))(keys)
    return perms.reshape(OWNERS * ROWS_DEV, MAXP).astype(jnp.int32)


def drawn_draws(key):
    pool = jax.random.normal(jax.random.fold_in(key, 12), (OWNERS * RES_PAGES, PAGE, 2 * KV * HD), jnp.float32)
    queries = jax.random.normal(jax.random.fold_in(key, 13), (ROWS_TOTAL, H * HD), jnp.float32)
    return (pool, queries)


def draw_block_table(key, part):
    return page_table(key)


def draw_kv_pool(key, part):
    return drawn_draws(key)[0].astype(jnp.bfloat16)


def draw_queries(key, part):
    return drawn_draws(key)[1].astype(jnp.bfloat16)


def place_ends(drawn, stream_key, smallest, largest):
    longest = drawn.shape.index(max(drawn.shape))
    spots = []
    for shift in (0, 1):
        where = [jax.random.randint(jax.random.fold_in(stream_key, axis), (), 0, length) for axis, length in enumerate(drawn.shape)]
        where[longest] = (where[longest] + shift) % drawn.shape[longest]
        spots.append(tuple(where))
    return drawn.at[spots[0]].set(smallest).at[spots[1]].set(largest)


def block_scale(stream_key, dims, shards, smallest, high):
    factor_of = 1.0
    for axis_at, shards_of in shards:
        heights = jax.random.uniform(jax.random.fold_in(jax.random.fold_in(stream_key, 6), axis_at), (shards_of,), jnp.float32, smallest / len(shards), high / len(shards))
        factor_of = factor_of * jnp.repeat(jnp.exp(heights), dims[axis_at] // shards_of).reshape((-1,) + (1,) * (len(dims) - 1 - axis_at))
    return factor_of


def routed_block(rng, own, number, rows, amount, top, bound, lean):
    sequence = jax.random.permutation(rng, amount)
    packed, common = shares(amount, rows * top, bound, lean, True), shares(amount, rows * top, bound, lean, False)
    places = jnp.arange(amount)

    def named(tallies, rotation):
        used = int((tallies > 0).sum())
        fixed = max(1, used // 4)
        moved = fixed + (places - fixed + rotation * (used - fixed)) % max(1, amount - fixed)
        return jnp.zeros((amount,), jnp.int32).at[sequence[jnp.where(places < fixed, places, moved)]].set(jnp.asarray(tallies, jnp.int32))

    tallies = jnp.where(number % 4 == 0, named(packed, number // 4), named(common, number - number // 4 - 1))
    mixed = jax.random.permutation(jax.random.fold_in(own, 3), amount)
    giver, taker = mixed[0:amount // 2 * 2:2], mixed[1:amount // 2 * 2:2]
    margin = jnp.minimum(tallies[giver] - 1, bound - tallies[taker]) // 2
    margin = jnp.where((giver == sequence[0]) | (taker == sequence[0]) | (tallies[taker] == 0), 0, jnp.maximum(margin, 0))
    moved = jax.random.randint(jax.random.fold_in(own, 4), (amount // 2,), 0, 1 << 20) % (margin + 1)
    tallies = tallies.at[giver].add(-moved).at[taker].add(moved)
    members = jnp.searchsorted(jnp.cumsum(tallies), jnp.arange(rows * top), side="right").astype(jnp.int32)
    grid = members.reshape(top, rows).T
    grid = grid[jax.random.permutation(jax.random.fold_in(own, 1), rows)]
    rotation = jax.random.randint(jax.random.fold_in(own, 2), (rows, 1), 0, top)
    return jnp.take_along_axis(grid, (jnp.arange(top)[None, :] + rotation) % top, axis=1)


def shares(amount, total, limit, skew, full):
    portions = [(1 << 20) // math.isqrt(grade ** skew) + 1 for grade in range(1, amount + 1)]
    largest = limit if full else min(limit, max(-(-total // amount), total * portions[0] // sum(portions)))
    least = 1 if total - largest >= amount - 1 else 0
    counts, surplus = [largest] + [least] * (amount - 1), total - largest - least * (amount - 1)
    while surplus > 0:
        movable = [i for i in range(1, amount) if counts[i] < largest] or [i for i in range(1, amount) if counts[i] < limit]
        whole, remaining = sum([portions[i] for i in movable]), surplus
        for i in movable:
            extra = min(limit - counts[i], max(1, remaining * portions[i] // whole), surplus)
            counts[i] = counts[i] + extra
            surplus = surplus - extra
    return np.array(counts)


def bell_draw(key, dims, spread, most, shards=(), kind=jnp.bfloat16):
    entries = jax.random.normal(key, dims, jnp.float32) * spread
    if len(shards) > 0:
        entries = block_scale(key, dims, shards, -0.22, 0.18) * entries
    return jnp.clip(entries, min=-most, max=most).astype(kind)


def setup_inputs(seed: int = 0) -> dict:
    splits = jax.random.split(jax.random.key(seed), 11)
    tokens = bell_draw(splits[0], (TOKENS, D), 1.0, 6.0, ((0, 32), (1, 8)))
    norm_gain = jnp.clip(1.0 + 0.18 * jax.random.normal(splits[1], (D,), jnp.float32), 0.099609375, 1.8984375).astype(jnp.bfloat16)
    kv_weight = bell_draw(splits[2], (D, 2 * KV * HD), D ** -0.5, 0.0625, ((0, 8),))
    page_dest_keys = jax.random.split(jax.random.fold_in(splits[3], 1), NEWPAGES // PAGES_DEV)
    page_dest_turns = jax.random.permutation(jax.random.fold_in(splits[3], 3), NEWPAGES // PAGES_DEV)
    page_dest = jax.vmap(lambda own, number: routed_block(jax.random.fold_in(splits[3], 2), own, number, PAGES_DEV, OWNERS, 1, SLOT, 2))(page_dest_keys, page_dest_turns).reshape((NEWPAGES, 1))
    page_row = place_ends(jax.random.randint(splits[4], (NEWPAGES,), 0, ROWS_DEV), jax.random.fold_in(splits[4], 1), 0, ROWS_DEV - 1).astype(jnp.int32)
    queries = draw_queries(jax.random.fold_in(splits[10], 71), 0)
    kv_pool = draw_kv_pool(jax.random.fold_in(splits[10], 71), 0)
    block_table = draw_block_table(jax.random.fold_in(splits[10], 71), 0)
    ctx_len = place_ends(jax.random.randint(splits[8], (ROWS_TOTAL,), 2, MAXP * PAGE + 1), jax.random.fold_in(splits[8], 1), 2, MAXP * PAGE).astype(jnp.int32)
    new_kv = bell_draw(splits[9], (ROWS_TOTAL, 2 * KV * HD), 1.0, 6.0, ((0, 32), (1, 8)))
    return {"tokens": tokens, "norm_gain": norm_gain, "kv_weight": kv_weight, "page_dest": page_dest, "page_row": page_row, "queries": queries, "kv_pool": kv_pool, "block_table": block_table, "ctx_len": ctx_len, "new_kv": new_kv}


EPS = 1e-06

def attend(queries, resident, res_mask, incoming, inc_mask, own):
    scale = HD ** (-0.5)
    q = queries.astype(jnp.float32)
    res = resident.astype(jnp.float32)
    inc = incoming.astype(jnp.float32)
    mine = own.astype(jnp.float32)
    s_res = jnp.einsum('rgjd,rtgd->rgjt', q, res[:, :, :, 0, :]) * scale
    s_inc = jnp.einsum('rgjd,sgd->rgjs', q, inc[:, :, 0, :]) * scale
    s_own = jnp.einsum('rgjd,rgd->rgj', q, mine[:, :, 0, :]) * scale
    m_res = res_mask[:, None, None, :]
    m_inc = inc_mask[:, None, None, :]
    top = jnp.maximum(lax.optimization_barrier(jnp.max(jnp.where(m_res, s_res, -jnp.inf), axis=3)), lax.optimization_barrier(jnp.max(jnp.where(m_inc, s_inc, -jnp.inf), axis=3)))
    top = jnp.maximum(top, s_own)
    e_res = jnp.where(m_res, jnp.exp(s_res - top[..., None]), 0.0)
    e_inc = jnp.where(m_inc, jnp.exp(s_inc - top[..., None]), 0.0)
    e_own = jnp.exp(s_own - top)
    total = lax.optimization_barrier(jnp.sum(e_res, axis=3)) + lax.optimization_barrier(jnp.sum(e_inc, axis=3)) + e_own
    p_res = (e_res / total[..., None]).astype(jnp.bfloat16).astype(jnp.float32)
    p_inc = (e_inc / total[..., None]).astype(jnp.bfloat16).astype(jnp.float32)
    p_own = (e_own / total).astype(jnp.bfloat16).astype(jnp.float32)
    out = jnp.einsum('rgjt,rtgd->rgjd', p_res, res[:, :, :, 1, :])
    out = out + jnp.einsum('rgjs,sgd->rgjd', p_inc, inc[:, :, 1, :])
    out = out + p_own[..., None] * mine[:, :, None, 1, :]
    return out.astype(jnp.bfloat16)

def reference(tokens, norm_gain, kv_weight, page_dest, page_row, queries, kv_pool, block_table, ctx_len, new_kv):
    wide = tokens.astype(jnp.float32)
    scale = lax.rsqrt(lax.optimization_barrier(jnp.mean(wide * wide, axis=1, keepdims=True)) + EPS)
    normed = (wide * scale * norm_gain.astype(jnp.float32)).astype(jnp.bfloat16)
    block_width = D // N_TP
    summed = jnp.zeros((TOKENS, 2 * KV * HD), jnp.float32)
    for block in range(N_TP):
        lower = block * block_width
        term = jnp.dot(normed[:, lower:lower + block_width], kv_weight[lower:lower + block_width], preferred_element_type=jnp.float32).astype(jnp.bfloat16)
        summed = summed + lax.optimization_barrier(term).astype(jnp.float32)
    fresh = summed.astype(jnp.bfloat16)
    pages = fresh.reshape(NEWPAGES, PAGE, 2 * KV * HD)
    target = page_dest[:, 0]
    capacity = OWNERS * SLOT
    group = H // KV

    def one_owner(item):
        owner, q_own, pool_own, table_own, length_own, kv_own = item
        order = jnp.argsort((target != owner).astype(jnp.int32), stable=True)[:capacity]
        live = target[order] == owner
        labels = jnp.where(live, page_row[order] + 1, 0).astype(jnp.int32)
        incoming = pages[order].reshape(capacity * PAGE, KV, 2, HD)
        token_tags = jnp.repeat(labels, PAGE)
        inc_mask = token_tags[None, :] == (jnp.arange(ROWS_DEV, dtype=jnp.int32) + 1)[:, None]
        resident = pool_own[table_own].reshape(ROWS_DEV, MAXP * PAGE, KV, 2, HD)
        res_mask = jnp.arange(MAXP * PAGE, dtype=jnp.int32)[None, :] < length_own[:, None]
        result = attend(q_own.reshape(ROWS_DEV, KV, group, HD), resident, res_mask, incoming, inc_mask, kv_own.reshape(ROWS_DEV, KV, 2, HD))
        return result.reshape(ROWS_DEV, H * HD)
    outputs = lax.map(one_owner, (jnp.arange(OWNERS, dtype=jnp.int32), queries.reshape(OWNERS, ROWS_DEV, H * HD), kv_pool.reshape(OWNERS, RES_PAGES, PAGE, 2 * KV * HD), block_table.reshape(OWNERS, ROWS_DEV, MAXP), ctx_len.reshape(OWNERS, ROWS_DEV), new_kv.reshape(OWNERS, ROWS_DEV, 2 * KV * HD)))
    return outputs.reshape(ROWS_TOTAL, H * HD)
```

```python
import jax
import jax.numpy as jnp
from jax import lax
from jax.experimental import pallas as pl
from jax.experimental.pallas import tpu as pltpu
from jax.sharding import Mesh
from jax.sharding import PartitionSpec as P

HD = 128
PAGE = 16
MAXP = 4
SLOT = 4
EPS = 1e-06
OWN = ("section", "rep")
NEAR = ((0, 1), (1, 0), (2, 3), (3, 2))
FAR = ((0, 3), (3, 0), (1, 2), (2, 1))
SWAP = ((0, 1), (1, 0))
F32 = jnp.float32
BF = jnp.bfloat16


def nt(a, b):
    return lax.dot_general(a, b, (((1,), (1,)), ((), ())), preferred_element_type=F32)


def first_kernel(order, tok, gain, w0, w1, w2, w3, oa, ob, oss, wcat, ssq):
    m = pl.program_id(0)
    rows = tok.shape[0]
    tokens = wcat.shape[0]

    @pl.when(m == 0)
    def _():
        for k, w in enumerate((w0, w1, w2, w3)):
            wcat[:, k * HD : (k + 1) * HD] = w[...]

    x = tok[...].astype(F32)
    xg = (x * gain[...].astype(F32)).astype(BF)
    r = jnp.dot(xg, wcat[...], preferred_element_type=F32).astype(BF)
    at = pl.ds(pl.multiple_of(m * rows, rows), rows)
    for k in range(2):
        oa[k, at, :] = r[:, k * HD : (k + 1) * HD]
        ob[k, at, :] = r[:, (k + 2) * HD : (k + 3) * HD]
    ssq[:, at] = nt(jnp.ones((8, x.shape[1]), BF), (x * x).astype(BF))

    @pl.when(m == pl.num_programs(0) - 1)
    def _():
        n = ssq.shape[1] // HD
        parts = [ssq[0:1, i * HD : (i + 1) * HD] for i in range(n)]
        tile = jnp.concatenate(parts + [jnp.zeros((16 - n, HD), F32)], axis=0).astype(BF)
        oss[...] = tile
        for k in range(2):
            oa[k, ssq.shape[1] : ssq.shape[1] + 16, :] = tile
            ob[k, ssq.shape[1] : ssq.shape[1] + 16, :] = tile


def rest_kernel(order, tok, gain, ss, *refs):
    ws, outs, wcat = refs[:12], refs[12:20], refs[20]
    m = pl.program_id(0)
    rows = tok.shape[0]

    @pl.when(m == 0)
    def _():
        for k, w in enumerate(ws):
            wcat[:, k * HD : (k + 1) * HD] = w[...]
        for o in (outs[4], outs[5]):
            n = o.shape[1] - 16
            for k in range(2):
                o[k, n : n + 16, :] = ss[...]

    x = tok[...].astype(F32)
    xg = (x * gain[...].astype(F32)).astype(BF)
    r = jnp.dot(xg, wcat[...], preferred_element_type=F32).astype(BF)
    at = pl.ds(pl.multiple_of(m * rows, rows), rows)
    for k in range(4):
        outs[k][at, :] = r[:, k * HD : (k + 1) * HD]
    for k in range(8):
        outs[4 + k // 2][k % 2, at, :] = r[:, (k + 4) * HD : (k + 5) * HD]


def project(tokens, gain, weight, order_a, order_b):
    n, d = tokens.shape
    rows = n // 4
    col = lambda k: pl.BlockSpec((d, HD), lambda m, order: (0, order[k]))
    whole = lambda s: pl.BlockSpec(s, lambda m, order: (0,) * len(s))
    tspec = pl.BlockSpec((rows, d), lambda m, order: (m, 0))
    gspec = whole((1, d))
    big, mid, small = (2, n + 16, HD), (2, n, HD), (n, HD)
    limit = pltpu.CompilerParams(dimension_semantics=("arbitrary",), vmem_limit_bytes=48 << 20)
    sa, sb, ss = pl.pallas_call(
        first_kernel,
        grid_spec=pltpu.PrefetchScalarGridSpec(
            num_scalar_prefetch=1,
            grid=(4,),
            in_specs=[tspec, gspec] + [col(k) for k in range(4)],
            out_specs=[whole(big), whole(big), whole((16, HD))],
            scratch_shapes=[pltpu.VMEM((d, 4 * HD), BF), pltpu.VMEM((8, n), F32)],
        ),
        out_shape=[jax.ShapeDtypeStruct(s, BF) for s in (big, big, (16, HD))],
        compiler_params=limit,
        name="project_first",
    )(order_a, tokens, gain, weight, weight, weight, weight)
    shapes = [small] * 4 + [big, big, mid, mid]
    rest = pl.pallas_call(
        rest_kernel,
        grid_spec=pltpu.PrefetchScalarGridSpec(
            num_scalar_prefetch=1,
            grid=(4,),
            in_specs=[tspec, gspec, whole((16, HD))] + [col(k) for k in range(12)],
            out_specs=[whole(s) for s in shapes],
            scratch_shapes=[pltpu.VMEM((d, 12 * HD), BF)],
        ),
        out_shape=[jax.ShapeDtypeStruct(s, BF) for s in shapes],
        compiler_params=limit,
        name="project_rest",
    )(order_b, tokens, gain, ss, *([weight] * 12))
    return sa, sb, rest


def split3(x):
    hi = x.astype(BF)
    left = x - hi.astype(F32)
    mid = left.astype(BF)
    low = (left - mid.astype(F32)).astype(BF)
    return hi, mid, low


def page_group(x, op):
    lane = lax.broadcasted_iota(jnp.int32, x.shape, 1)
    n = x.shape[1]
    for k in (1, 2, 4, 8):
        other = jnp.where((lane & k) == 0, pltpu.roll(x, n - k, 1), pltpu.roll(x, k, 1))
        x = op(x, other)
    return x


def score_kernel(keys, qall, where_page, dest_col, dest_row, tag, probs, ext, psel, qp):
    n = keys.shape[0] - 16
    pages = n // PAGE
    owners_rows = qall.shape[0]
    pick = (
        lax.broadcasted_iota(jnp.int32, (pages, owners_rows), 1) == where_page[...]
    ).astype(BF)
    qp[...] = jnp.dot(pick, qall[...], preferred_element_type=F32)
    block = 256
    bp = block // PAGE
    ssum = keys[n : n + 16, :].astype(F32)
    lses = []
    for b in range(n // block):
        q = jnp.concatenate(
            [qp[b * bp : (b + 1) * bp, j * HD : (j + 1) * HD] for j in range(8)], axis=0
        ).astype(BF)
        s = nt(q, keys[b * block : (b + 1) * block, :]).reshape(8, bp, block)
        own = (
            lax.broadcasted_iota(jnp.int32, (bp, block), 1) // PAGE
            == lax.broadcasted_iota(jnp.int32, (bp, block), 0)
        )
        s = jnp.sum(jnp.where(own[None], s, 0.0), axis=1)
        total = jnp.concatenate(
            [ssum[2 * b : 2 * b + 1, :], ssum[2 * b + 1 : 2 * b + 2, :]], axis=1
        )
        scale = lax.rsqrt(total / 8192.0 + EPS)
        s = s * (scale * HD ** (-0.5))
        top = page_group(s, jnp.maximum)
        e = jnp.exp(s - top)
        mass = page_group(e, jnp.add)
        probs[:, b * block : (b + 1) * block] = e / mass * scale
        lses.append(top + jnp.log(mass))
    lse = jnp.concatenate(lses, axis=1)
    hi, mid, low = split3(lse)
    tags = jnp.broadcast_to(tag[...], (8, n))
    stack = jnp.concatenate(
        [hi.astype(F32), mid.astype(F32), low.astype(F32), tags, jnp.zeros((HD - 32, n), F32)], axis=0
    ).astype(BF)
    p0 = lax.broadcasted_iota(jnp.int32, (pages, pages), 0)
    p1 = lax.broadcasted_iota(jnp.int32, (pages, pages), 1)
    same = (dest_col[...] == dest_row[...]) & (p0 < p1)
    rank = jnp.sum(same.astype(F32), axis=0, keepdims=True)
    place = dest_row[...].astype(F32) * SLOT + rank
    slots = psel.shape[0]
    sel = lax.broadcasted_iota(jnp.int32, (slots, pages), 0).astype(F32) == place
    sel = sel.astype(F32).astype(BF)
    psel[...] = sel
    head = (
        lax.broadcasted_iota(jnp.int32, (pages, n), 1)
        == lax.broadcasted_iota(jnp.int32, (pages, n), 0) * PAGE
    ).astype(F32).astype(BF)
    wide = jnp.dot(sel, head, preferred_element_type=F32).astype(BF)
    ext[...] = nt(wide, stack).astype(BF)


def score(keys, qall, where_page, dest_col, dest_row, tag, slots):
    n = keys.shape[0] - 16
    return pl.pallas_call(
        score_kernel,
        out_shape=[
            jax.ShapeDtypeStruct((8, n), F32),
            jax.ShapeDtypeStruct((slots, HD), BF),
            jax.ShapeDtypeStruct((slots, n // PAGE), BF),
        ],
        scratch_shapes=[pltpu.VMEM((n // PAGE, qall.shape[1]), F32)],
        name="score",
    )(keys, qall, where_page, dest_col, dest_row, tag)


def value_kernel(values, probs, ext, psel, out, acc):
    n = values.shape[0]
    block = 256
    bp = block // PAGE
    own = (
        lax.broadcasted_iota(jnp.int32, (bp, block), 1) // PAGE
        == lax.broadcasted_iota(jnp.int32, (bp, block), 0)
    )
    for b in range(n // block):
        p = probs[:, b * block : (b + 1) * block]
        a = jnp.concatenate(
            [jnp.where(own, p[j : j + 1, :], 0.0) for j in range(8)], axis=0
        ).astype(BF)
        o = jnp.dot(a, values[b * block : (b + 1) * block, :], preferred_element_type=F32)
        for j in range(8):
            acc[b * bp : (b + 1) * bp, j * HD : (j + 1) * HD] = o[j * bp : (j + 1) * bp].astype(BF)
    width = acc.shape[1]
    out[:, :width] = jnp.dot(psel[...], acc[...], preferred_element_type=F32).astype(BF)
    out[:, width:] = ext[...]


def value(values, probs, ext, psel):
    slots = psel.shape[0]
    return pl.pallas_call(
        value_kernel,
        out_shape=jax.ShapeDtypeStruct((slots, 9 * HD), BF),
        scratch_shapes=[pltpu.VMEM((psel.shape[1], 8 * HD), BF)],
        name="value",
    )(values, probs, ext, psel)


def resident_kernel(queries, pool, table, length, fresh, top_out, mass_out, acc_out):
    rows = queries.shape[0]
    pages = table.shape[1] * rows
    n = pool.shape[0]
    q32 = queries[...].astype(F32)
    q = jnp.concatenate([q32[:, j * HD : (j + 1) * HD] for j in range(8)], axis=0)
    s = nt(q.astype(BF), pool[:, :HD]) * HD ** (-0.5)
    token = lax.broadcasted_iota(jnp.int32, (rows, n), 1)
    valid = jnp.zeros((rows, n), jnp.int32)
    for i in range(table.shape[1]):
        left = length[...] - PAGE * i
        hit = (token // PAGE == table[:, i : i + 1]) & (token % PAGE < left)
        valid = valid + hit.astype(jnp.int32)
    mask = jnp.concatenate([valid] * 8, axis=0) > 0
    own = fresh[...].astype(F32)
    own_k = jnp.concatenate([own[:, :HD]] * 8, axis=0)
    own_v = jnp.concatenate([own[:, HD:]] * 8, axis=0)
    s_own = jnp.sum(q * own_k, axis=1, keepdims=True) * HD ** (-0.5)
    top = jnp.maximum(jnp.max(jnp.where(mask, s, -jnp.inf), axis=1, keepdims=True), s_own)
    e = jnp.where(mask, jnp.exp(s - top), 0.0)
    e_own = jnp.exp(s_own - top)
    top_out[...] = top
    mass_out[...] = jnp.sum(e, axis=1, keepdims=True) + e_own
    acc_out[...] = (
        jnp.dot(e.astype(BF), pool[:, HD:], preferred_element_type=F32) + e_own * own_v
    )


def resident(queries, pool, table, length, fresh):
    n = queries.shape[0] * 8
    return pl.pallas_call(
        resident_kernel,
        out_shape=[
            jax.ShapeDtypeStruct((n, 1), F32),
            jax.ShapeDtypeStruct((n, 1), F32),
            jax.ShapeDtypeStruct((n, HD), F32),
        ],
        name="resident",
    )(queries, pool, table, length, fresh)


def merge_kernel(got, top_in, mass_in, acc_in, out):
    rows = out.shape[0]
    slots = got.shape[0]
    ext = got[:, 8 * HD :].astype(F32).T
    lse = ext[0:8] + ext[8:16] + ext[16:24]
    mask = ext[24:25] == (lax.broadcasted_iota(jnp.int32, (rows, slots), 0) + 1).astype(F32)
    for j in range(8):
        at = slice(j * rows, (j + 1) * rows)
        l = jnp.where(mask, lse[j : j + 1], -jnp.inf)
        top = jnp.maximum(jnp.max(l, axis=1, keepdims=True), top_in[at, :])
        w = jnp.where(mask, jnp.exp(l - top), 0.0)
        keep = jnp.exp(top_in[at, :] - top)
        total = jnp.sum(w, axis=1, keepdims=True) + mass_in[at, :] * keep
        o = jnp.dot(w.astype(BF), got[:, j * HD : (j + 1) * HD], preferred_element_type=F32)
        out[:, j * HD : (j + 1) * HD] = ((o + acc_in[at, :] * keep) / total).astype(BF)


def merge(got, top, mass, acc, rows):
    return pl.pallas_call(
        merge_kernel,
        out_shape=jax.ShapeDtypeStruct((rows, 8 * HD), BF),
        name="merge",
    )(got, top, mass, acc)


def body(
    tokens,
    norm_gain,
    kv_weight,
    page_dest,
    page_row,
    queries,
    kv_pool,
    block_table,
    ctx_len,
    new_kv,
):
    x = lax.axis_index("tp_1")
    high = lax.axis_index("tp_0")
    near, far = x ^ 1, 3 - x
    a_send = [3 - near, near]
    b_send = [4 + (far ^ 1), 4 + far]
    a_keep = [3 - x, x]
    b_keep = [4 + near, 4 + x]
    cols = lambda hs, kv: [2 * h + kv for h in hs]
    order_a = jnp.stack(cols(a_send, 0) + cols(b_send, 0)).astype(jnp.int32)
    order_b = jnp.stack(
        cols(a_send, 1) + cols(b_send, 1) + cols(a_keep, 0) + cols(b_keep, 0) + cols(a_keep, 1) + cols(b_keep, 1)
    ).astype(jnp.int32)
    ks_a, ks_b, rest = project(tokens, norm_gain.reshape(1, -1), kv_weight, order_a, order_b)
    vf_a, vo_a, vf_b, vo_b, kk_a, kk_b, vk_a, vk_b = rest
    move = lambda v, pairs: lax.ppermute(v, "tp_1", pairs)
    k1_a, k1_b = move(ks_a, NEAR), move(ks_b, FAR)
    v1f_a, v1f_b = move(vf_a, NEAR), move(vf_b, FAR)

    owners = lax.axis_size(OWN)
    rows = queries.shape[0]
    qall = lax.all_to_all(
        jnp.broadcast_to(queries[None], (owners, *queries.shape)), OWN, 0, 0, tiled=True
    ).reshape(owners * rows, queries.shape[1])

    k2_a, k2_b, vo_a, vo_b = lax.optimization_barrier(
        (k1_a[0] + kk_a[0], k1_b[0] + kk_b[0], vo_a, vo_b)
    )
    k2_a, k2_b = move(k2_a, FAR), move(k2_b, NEAR)
    v1o_a, v1o_b = move(vo_a, NEAR), move(vo_b, FAR)
    v2_a, v2_b = move(v1f_a + vk_a[0], FAR), move(v1f_b + vk_b[0], NEAR)

    first = high == 0
    swap = lambda v: lax.ppermute(v, "tp_0", SWAP)
    ksum_a, ksum_b = k1_a[1] + kk_a[1] + k2_a, k1_b[1] + kk_b[1] + k2_b
    keys = swap(jnp.where(first, ksum_b, ksum_a)) + jnp.where(first, ksum_a, ksum_b)
    vsum_a, vsum_b = v1o_a + vk_a[1] + v2_a, v1o_b + vk_b[1] + v2_b
    values = swap(jnp.where(first, vsum_b, vsum_a)) + jnp.where(first, vsum_a, vsum_b)

    pages = page_row.shape[0]
    where_page = page_dest * rows + page_row.reshape(pages, 1)
    tag = jnp.repeat((page_row + 1).astype(F32), PAGE).reshape(1, -1)
    probs, ext, psel = score(
        keys, qall, where_page, page_dest, page_dest.reshape(1, pages), tag, owners * SLOT
    )
    sent = value(values, probs, ext, psel)
    got = lax.all_to_all(sent.reshape(owners, SLOT, -1), OWN, 0, 0, tiled=True)
    top, mass, acc = resident(
        queries,
        kv_pool.reshape(-1, kv_pool.shape[2]),
        block_table,
        ctx_len.reshape(rows, 1),
        new_kv,
    )
    return merge(got.reshape(owners * SLOT, -1), top, mass, acc, rows)


def solution(mesh):
    split = Mesh(
        mesh.devices.reshape(mesh.shape["section"], mesh.shape["rep"], 2, 4),
        ("section", "rep", "tp_0", "tp_1"),
    )
    tp = ("tp_0", "tp_1")
    placed = (
        P(OWN, tp),
        P(tp),
        P(tp, None),
        P(OWN, None),
        P(OWN),
        P(OWN, tp),
        P(OWN, None, tp),
        P(OWN, None),
        P(OWN),
        P(OWN, tp),
    )
    return jax.shard_map(body, mesh=split, in_specs=placed, out_specs=P(OWN, tp), check_vma=False)
```

```python
import jax
import jax.numpy as jnp
from jax import lax
from jax.experimental import pallas as pl
from jax.experimental.pallas import tpu as pltpu
from jax.sharding import Mesh
from jax.sharding import PartitionSpec as P

HD = 128
PAGE = 16
SLOT = 4
EPS = 1e-06
OWN = ("section", "rep")
NEAR = ((0, 1), (1, 0), (2, 3), (3, 2))
FAR = ((0, 3), (3, 0), (1, 2), (2, 1))
SWAP = ((0, 1), (1, 0))
F32 = jnp.float32
BF = jnp.bfloat16


def nt(a, b):
    return lax.dot_general(a, b, (((1,), (1,)), ((), ())), preferred_element_type=F32)


def blocks_for(names):
    x = lax.axis_index("tp_1")
    near, far = x ^ 1, 3 - x
    heads = {
        "a_send": (3 - near, near),
        "b_send": (4 + (far ^ 1), 4 + far),
        "a_keep": (3 - x, x),
        "b_keep": (4 + near, 4 + x),
    }
    return [2 * h + kv for name, kv in names for h in heads[name]]


def load_all(names, tok, w, tokv, wv, tsem, wsem):
    rows = tokv.shape[0] // tsem.shape[0]
    fetch = [
        pltpu.make_async_copy(
            w.at[:, pl.ds(pl.multiple_of(c * HD, HD), HD)], wv.at[:, k * HD : (k + 1) * HD], wsem.at[k]
        )
        for k, c in enumerate(blocks_for(names))
    ]
    chunks = [
        pltpu.make_async_copy(
            tok.at[m * rows : (m + 1) * rows, :], tokv.at[m * rows : (m + 1) * rows, :], tsem.at[m]
        )
        for m in range(tsem.shape[0])
    ]
    for c in chunks[:1] + fetch[:4] + chunks[1:] + fetch[4:]:
        c.start()
    return fetch, chunks, rows


NAMES = (
    ("a_send", 0), ("b_send", 0), ("a_send", 1), ("b_send", 1),
    ("a_keep", 0), ("b_keep", 0), ("a_keep", 1), ("b_keep", 1),
)


def project_kernel(tok, gain, w, *refs):
    outs = refs[:16]
    tokv, wv, obuf, ssq, gainv, tsem, wsem, osem, gsem = refs[16:]
    early = pltpu.make_async_copy(gain, gainv, gsem)
    early.start()
    fetch, chunks, rows = load_all(NAMES, tok, w, tokv, wv, tsem, wsem)
    n, d = tokv.shape
    early.wait()
    g = gainv[...].astype(F32).reshape(1, -1)
    done = []

    def ship(k):
        c = pltpu.make_async_copy(obuf.at[k, 0 : outs[k].shape[0], :], outs[k], osem.at[k])
        c.start()
        done.append(c)

    for k in range(0, 16, 4):
        for m, c in enumerate(chunks):
            at = slice(m * rows, (m + 1) * rows)
            if k == 0:
                c.wait()
                x = tokv[at, :].astype(F32)
                tokv[at, :] = (x * g).astype(BF)
                sq = x * x
                part = sum(sq[:, i : i + HD] for i in range(0, d, HD))
                ssq[:, at] = nt(jnp.ones((8, HD), BF), part.astype(BF))
            if m == 0:
                for f in fetch[k : k + 4]:
                    f.wait()
            r = jnp.dot(tokv[at, :], wv[:, k * HD : (k + 4) * HD], preferred_element_type=F32).astype(BF)
            for i in range(4):
                if k < 8:
                    obuf[k + i, at, :] = r[:, i * HD : (i + 1) * HD]
                else:
                    outs[k + i][at, :] = r[:, i * HD : (i + 1) * HD]
        if k == 0:
            parts = [ssq[0:1, i * HD : (i + 1) * HD] for i in range(n // HD)]
            tile = jnp.concatenate(parts + [jnp.zeros((16 - n // HD, HD), F32)], axis=0).astype(BF)
            for i in range(4):
                obuf[i, n : n + 16, :] = tile
                outs[8 + i][n : n + 16, :] = tile
        if k < 8:
            for i in range(4):
                ship(k + i)
    for c in done:
        c.wait()


VM = 48 << 20


def projection(kernel, count, chunks, tokens, gain, weight, extra, shapes, scratch, outs, sems):
    n, d = tokens.shape
    hbm = pl.BlockSpec(memory_space=pltpu.HBM)
    vmem = pl.BlockSpec(memory_space=pltpu.VMEM)
    return pl.pallas_call(
        kernel,
        in_specs=[hbm, hbm, hbm] + [vmem for _ in extra],
        out_specs=outs,
        scratch_shapes=[pltpu.VMEM((n, d), BF), pltpu.VMEM((d, count * HD), BF)]
        + scratch
        + [pltpu.SemaphoreType.DMA((chunks,)), pltpu.SemaphoreType.DMA((count,))]
        + sems,
        out_shape=[jax.ShapeDtypeStruct(s, BF) for s in shapes],
        compiler_params=pltpu.CompilerParams(vmem_limit_bytes=VM),
    )(tokens, gain, weight, *extra)


def pair_kernel(a0, a1, b0, b1, oa, ob):
    oa[...] = a0[...] + a1[...]
    ob[...] = b0[...] + b1[...]


def pair_sum(a0, a1, b0, b1):
    return pl.pallas_call(
        pair_kernel, out_shape=[jax.ShapeDtypeStruct(a0.shape, BF)] * 2, compiler_params=small()
    )(a0, a1, b0, b1)


def own_kernel(a0, a1, a2, b0, b1, b2, give, keep):
    first = (lax.axis_index("tp_0") == 0).astype(jnp.int32)
    a = (a0[...].astype(F32) + a1[...].astype(F32) + a2[...].astype(F32)).astype(BF)
    b = (b0[...].astype(F32) + b1[...].astype(F32) + b2[...].astype(F32)).astype(BF)

    @pl.when(first == 1)
    def _():
        give[...] = b
        keep[...] = a

    @pl.when(first == 0)
    def _():
        give[...] = a
        keep[...] = b


def own_sum(*parts):
    return pl.pallas_call(
        own_kernel,
        out_shape=[jax.ShapeDtypeStruct(parts[0].shape, BF)] * 2,
        compiler_params=small(8),
    )(*parts)


def split3(x):
    hi = x.astype(BF)
    left = x - hi.astype(F32)
    mid = left.astype(BF)
    low = (left - mid.astype(F32)).astype(BF)
    return hi, mid, low


def page_group(x, op):
    lane = lax.broadcasted_iota(jnp.int32, x.shape, 1)
    n = x.shape[1]
    for k in (1, 2, 4, 8):
        other = jnp.where((lane & k) == 0, pltpu.roll(x, n - k, 1), pltpu.roll(x, k, 1))
        x = op(x, other)
    return x


def prepare_kernel(qown, qother, dest, row, mine, qpage, psel, wide, tags):
    pages = dest.shape[1]
    n = wide.shape[1]
    per_owner = 8
    dest_f, row_f = dest[...].astype(F32), row[...].astype(F32)
    p0 = lax.broadcasted_iota(jnp.int32, (pages, pages), 0)
    p1 = lax.broadcasted_iota(jnp.int32, (pages, pages), 1)
    column = lambda v: jnp.sum(jnp.where(p0 == p1, v, 0.0), axis=1, keepdims=True)
    dest_c = column(dest_f)
    half = qown.shape[0]
    place = (dest[...] ^ mine[0]).astype(F32)
    where_page = column(place * per_owner + row_f)
    lanes = lax.broadcasted_iota(jnp.int32, (pages, half), 1).astype(F32)
    pick = lambda shift: (lanes + shift == where_page).astype(F32).astype(BF)
    qp = jnp.dot(pick(0.0), qown[...], preferred_element_type=F32) + jnp.dot(
        pick(float(half)), qother[...], preferred_element_type=F32
    )
    bp = PAGE
    for b in range(pages // bp):
        for j in range(8):
            at = (b * 8 + j) * bp
            qpage[at : at + bp, :] = qp[b * bp : (b + 1) * bp, j * HD : (j + 1) * HD].astype(BF)
    rank = jnp.sum(((dest_c == dest_f) & (p0 < p1)).astype(F32), axis=0, keepdims=True)
    place = (dest_f * SLOT + rank) * 2
    slots = psel.shape[1]
    at = lax.broadcasted_iota(jnp.int32, (slots, pages), 0).astype(F32)
    even = (at == place).astype(F32)
    odd = (at == place + 1).astype(F32)
    psel[0] = even.astype(BF)
    psel[1] = odd.astype(BF)
    token = lax.broadcasted_iota(jnp.int32, (pages, n), 1)
    page = lax.broadcasted_iota(jnp.int32, (pages, n), 0)
    head = (token == page * PAGE).astype(F32).astype(BF)
    wide[...] = jnp.dot((even + odd).astype(BF), head, preferred_element_type=F32).astype(BF)
    inside = (token // PAGE == page).astype(F32).astype(BF)
    tag8 = jnp.broadcast_to(row_f + 1.0, (8, pages)).astype(BF)
    tags[...] = jnp.dot(tag8, inside, preferred_element_type=F32)


def small(mib=6):
    return pltpu.CompilerParams(vmem_limit_bytes=mib << 20)


def prepare(qown, qother, dest, row, mine, slots, n):
    pages = dest.shape[1]
    return pl.pallas_call(
        prepare_kernel,
        out_shape=[
            jax.ShapeDtypeStruct((pages * 8, HD), BF),
            jax.ShapeDtypeStruct((2, slots * 2, pages), BF),
            jax.ShapeDtypeStruct((slots * 2, n), BF),
            jax.ShapeDtypeStruct((8, n), F32),
        ],
        in_specs=[pl.BlockSpec(memory_space=pltpu.VMEM)] * 4 + [pl.BlockSpec(memory_space=pltpu.SMEM)],
        compiler_params=small(),
        name="prepare",
    )(qown, qother, dest, row, mine)


def score_kernel(keys0, keys1, qpage, wide, tags, probs, ext, keys):
    n = keys0.shape[0] - 16
    ssum = keys0[n : n + 16, :].astype(F32) + keys1[n : n + 16, :].astype(F32)
    keys[...] = keys0[0:n, :] + keys1[0:n, :]
    block = 256
    bp = block // PAGE
    own = (
        lax.broadcasted_iota(jnp.int32, (bp, block), 1) // PAGE
        == lax.broadcasted_iota(jnp.int32, (bp, block), 0)
    )
    parts = []
    for b in range(n // block):
        q = qpage[b * 8 * bp : (b + 1) * 8 * bp, :]
        s = nt(q, keys[b * block : (b + 1) * block, :]).reshape(8, bp, block)
        parts.append(jnp.sum(jnp.where(own[None], s, 0.0), axis=1))
    total = jnp.concatenate([ssum[i : i + 1, :] for i in range(n // HD)], axis=1)
    scale = lax.rsqrt(total / 8192.0 + EPS)
    s = jnp.concatenate(parts, axis=1) * (scale * HD ** (-0.5))
    top = page_group(s, jnp.maximum)
    e = jnp.exp(s - top)
    mass = page_group(e, jnp.add)
    probs[...] = e / mass * scale
    hi, mid, low = split3(top + jnp.log(mass))
    stack = jnp.concatenate(
        [hi.astype(F32), mid.astype(F32), low.astype(F32), tags[...], jnp.zeros((HD - 32, n), F32)], axis=0
    ).astype(BF)
    ext[...] = nt(wide[...], stack).astype(BF)


def score(keys0, keys1, qpage, wide, tags):
    n = keys0.shape[0] - 16
    return pl.pallas_call(
        score_kernel,
        out_shape=[
            jax.ShapeDtypeStruct((8, n), F32),
            jax.ShapeDtypeStruct((wide.shape[0], HD), BF),
        ],
        scratch_shapes=[pltpu.VMEM((n, HD), BF)],
        compiler_params=small(),
        name="score",
    )(keys0, keys1, qpage, wide, tags)


def value_kernel(values0, values1, probs, ext, psel, out, acc):
    n = values0.shape[0]
    block = 256
    bp = block // PAGE
    own = (
        lax.broadcasted_iota(jnp.int32, (bp, block), 1) // PAGE
        == lax.broadcasted_iota(jnp.int32, (bp, block), 0)
    )
    for b in range(n // block):
        p = probs[:, b * block : (b + 1) * block]
        a = jnp.concatenate(
            [jnp.where(own, p[j : j + 1, :], 0.0) for j in range(8)], axis=0
        ).astype(BF)
        at = slice(b * block, (b + 1) * block)
        o = jnp.dot(a, values0[at, :] + values1[at, :], preferred_element_type=F32)
        for j in range(8):
            acc[b * bp : (b + 1) * bp, j * HD : (j + 1) * HD] = o[j * bp : (j + 1) * bp].astype(BF)
    half = acc.shape[1] // 2
    out[:, :half] = (
        jnp.dot(psel[0], acc[:, :half], preferred_element_type=F32)
        + jnp.dot(psel[1], acc[:, half:], preferred_element_type=F32)
    ).astype(BF)
    out[:, half:] = ext[...]


def value(values0, values1, probs, ext, psel):
    return pl.pallas_call(
        value_kernel,
        out_shape=jax.ShapeDtypeStruct((psel.shape[1], 5 * HD), BF),
        scratch_shapes=[pltpu.VMEM((psel.shape[2], 8 * HD), BF)],
        compiler_params=small(),
        name="value",
    )(values0, values1, probs, ext, psel)


def resident_kernel(queries, pool, table, length, fresh, top_out, mass_out, acc_out):
    rows = queries.shape[0]
    n = pool.shape[0]
    q32 = queries[...].astype(F32)
    q = jnp.concatenate([q32[:, j * HD : (j + 1) * HD] for j in range(8)], axis=0)
    s = nt(q.astype(BF), pool[:, :HD]) * HD ** (-0.5)
    token = lax.broadcasted_iota(jnp.int32, (rows, n), 1)
    valid = jnp.zeros((rows, n), jnp.int32)
    r0 = lax.broadcasted_iota(jnp.int32, (rows, rows), 0)
    r1 = lax.broadcasted_iota(jnp.int32, (rows, rows), 1)
    column = lambda v: jnp.sum(jnp.where(r0 == r1, v, 0), axis=1, keepdims=True)
    long = column(length[...])
    for i in range(table.shape[0]):
        hit = (token // PAGE == column(table[i : i + 1, :])) & (token % PAGE < long - PAGE * i)
        valid = valid + hit.astype(jnp.int32)
    mask = jnp.concatenate([valid] * 8, axis=0) > 0
    own = fresh[...].astype(F32)
    own_k = jnp.concatenate([own[:, :HD]] * 8, axis=0)
    own_v = jnp.concatenate([own[:, HD:]] * 8, axis=0)
    s_own = jnp.sum(q * own_k, axis=1, keepdims=True) * HD ** (-0.5)
    top = jnp.maximum(jnp.max(jnp.where(mask, s, -jnp.inf), axis=1, keepdims=True), s_own)
    e = jnp.where(mask, jnp.exp(s - top), 0.0)
    e_own = jnp.exp(s_own - top)
    top_out[...] = top
    mass_out[...] = jnp.sum(e, axis=1, keepdims=True) + e_own
    acc_out[...] = (
        jnp.dot(e.astype(BF), pool[:, HD:], preferred_element_type=F32) + e_own * own_v
    )


def resident(queries, pool, table, length, fresh):
    n = queries.shape[0] * 8
    return pl.pallas_call(
        resident_kernel,
        out_shape=[
            jax.ShapeDtypeStruct((n, 1), F32),
            jax.ShapeDtypeStruct((n, 1), F32),
            jax.ShapeDtypeStruct((n, HD), F32),
        ],
        compiler_params=small(),
        name="resident",
    )(queries, pool, table, length, fresh)


def merge_kernel(got, top_in, mass_in, acc_in, out):
    rows = out.shape[0]
    slots = got.shape[0]
    ext = got[:, 4 * HD :].astype(F32).T
    lse = ext[0:8] + ext[8:16] + ext[16:24]
    live = ext[24:25] == (lax.broadcasted_iota(jnp.int32, (rows, slots), 0) + 1).astype(F32)
    odd = lax.broadcasted_iota(jnp.int32, (rows, slots), 1) % 2
    for j in range(8):
        mask = live & (odd == j // 4)
        at = slice(j * rows, (j + 1) * rows)
        l = jnp.where(mask, lse[j : j + 1], -jnp.inf)
        top = jnp.maximum(jnp.max(l, axis=1, keepdims=True), top_in[at, :])
        w = jnp.where(mask, jnp.exp(l - top), 0.0)
        keep = jnp.exp(top_in[at, :] - top)
        total = jnp.sum(w, axis=1, keepdims=True) + mass_in[at, :] * keep
        k = j % 4
        o = jnp.dot(w.astype(BF), got[:, k * HD : (k + 1) * HD], preferred_element_type=F32)
        out[:, j * HD : (j + 1) * HD] = ((o + acc_in[at, :] * keep) / total).astype(BF)


def merge(got, top, mass, acc, rows):
    return pl.pallas_call(
        merge_kernel,
        out_shape=jax.ShapeDtypeStruct((rows, 8 * HD), BF),
        compiler_params=small(),
        name="merge",
    )(got, top, mass, acc)


def body(
    tokens,
    norm_gain,
    kv_weight,
    page_dest,
    page_row,
    queries,
    kv_pool,
    block_table,
    ctx_len,
    new_kv,
):
    n, d = tokens.shape
    ext, one = (n + 16, HD), (n, HD)
    gain = norm_gain

    vmem, hbm = pl.BlockSpec(memory_space=pltpu.VMEM), pl.BlockSpec(memory_space=pltpu.HBM)
    (
        kf_a, ko_a, kf_b, ko_b, vf_a, vo_a, vf_b, vo_b,
        kkf_a, kko_a, kkf_b, kko_b, vkf_a, vko_a, vkf_b, vko_b,
    ) = projection(
        project_kernel, 16, 4, tokens, gain, kv_weight, [],
        [ext] * 4 + [one] * 4 + [ext] * 4 + [one] * 4,
        [pltpu.VMEM((8, *ext), BF), pltpu.VMEM((8, n), F32), pltpu.VMEM((d,), BF)], [hbm] * 8 + [vmem] * 8,
        [pltpu.SemaphoreType.DMA((8,)), pltpu.SemaphoreType.DMA],
    )
    k1f_a, k1f_b = lax.ppermute(kf_a, "tp_1", NEAR), lax.ppermute(kf_b, "tp_1", FAR)
    k1o_a, k1o_b = lax.ppermute(ko_a, "tp_1", NEAR), lax.ppermute(ko_b, "tp_1", FAR)
    s_a, s_b = pair_sum(k1f_a, kkf_a, k1f_b, kkf_b)
    k2_a, k2_b = lax.ppermute(s_a, "tp_1", FAR), lax.ppermute(s_b, "tp_1", NEAR)
    v1f_a, v1f_b = lax.ppermute(vf_a, "tp_1", NEAR), lax.ppermute(vf_b, "tp_1", FAR)
    v1o_a, v1o_b = lax.ppermute(vo_a, "tp_1", NEAR), lax.ppermute(vo_b, "tp_1", FAR)
    owners = lax.axis_size(OWN)
    rows = queries.shape[0]
    peers = lax.axis_size("rep")
    spread = jnp.broadcast_to(queries[None], (peers, *queries.shape))
    qown = lax.all_to_all(spread, "rep", 0, 0, tiled=True).reshape(peers * rows, -1)
    qother = lax.ppermute(qown, "section", SWAP)
    s_a, s_b = pair_sum(v1f_a, vkf_a, v1f_b, vkf_b)
    v2_a, v2_b = lax.ppermute(s_a, "tp_1", FAR), lax.ppermute(s_b, "tp_1", NEAR)
    give, keep = own_sum(k1o_a, kko_a, k2_a, k1o_b, kko_b, k2_b)
    keys = (lax.ppermute(give, "tp_0", SWAP), keep)
    give, keep = own_sum(v1o_a, vko_a, v2_a, v1o_b, vko_b, v2_b)
    values = (lax.ppermute(give, "tp_0", SWAP), keep)

    pages = page_row.shape[0]
    mine = lax.axis_index("section").astype(jnp.int32).reshape(1) * peers
    qpage, psel, wide, tags = prepare(
        qown, qother, page_dest.reshape(1, pages), page_row.reshape(1, pages), mine,
        owners * SLOT, n,
    )
    top, mass, acc = resident(
        queries,
        kv_pool.reshape(-1, kv_pool.shape[2]),
        block_table.T,
        ctx_len.reshape(1, rows),
        new_kv,
    )
    probs, ext = score(*keys, qpage, wide, tags)
    sent = value(*values, probs, ext, psel)
    got = lax.all_to_all(sent.reshape(owners, 2 * SLOT, -1), OWN, 0, 0, tiled=True)
    return merge(got.reshape(owners * SLOT * 2, -1), top, mass, acc, rows)


def solution(mesh):
    split = Mesh(
        mesh.devices.reshape(mesh.shape["section"], mesh.shape["rep"], 2, 4),
        ("section", "rep", "tp_0", "tp_1"),
    )
    tp = ("tp_0", "tp_1")
    placed = (
        P(OWN, tp),
        P(tp),
        P(tp, None),
        P(OWN, None),
        P(OWN),
        P(OWN, tp),
        P(OWN, None, tp),
        P(OWN, None),
        P(OWN),
        P(OWN, tp),
    )

    return jax.shard_map(body, mesh=split, in_specs=placed, out_specs=P(OWN, tp), check_vma=False)
```

```python
import jax
import jax.numpy as jnp
from jax import lax
from jax.experimental import pallas as pl
from jax.experimental.pallas import tpu as pltpu
from jax.sharding import Mesh
from jax.sharding import PartitionSpec as P

HD = 128
PAGE = 16
SLOT = 4
EPS = 1e-06
OWN = ("section", "rep")
NEAR = ((0, 1), (1, 0), (2, 3), (3, 2))
FAR = ((0, 3), (3, 0), (1, 2), (2, 1))
SWAP = ((0, 1), (1, 0))
F32 = jnp.float32
BF = jnp.bfloat16


def nt(a, b):
    return lax.dot_general(a, b, (((1,), (1,)), ((), ())), preferred_element_type=F32)


def blocks_for(names):
    x = lax.axis_index("tp_1")
    near, far = x ^ 1, 3 - x
    heads = {
        "a_send": (3 - near, near),
        "b_send": (4 + (far ^ 1), 4 + far),
        "a_keep": (3 - x, x),
        "b_keep": (4 + near, 4 + x),
    }
    return [2 * h + kv for name, kv in names for h in heads[name]]


def load_all(names, tok, w, tokv, wv, tsem, wsem):
    rows = tokv.shape[0] // tsem.shape[0]
    fetch = [
        pltpu.make_async_copy(
            w.at[:, pl.ds(pl.multiple_of(c * HD, HD), HD)], wv.at[:, k * HD : (k + 1) * HD], wsem.at[k]
        )
        for k, c in enumerate(blocks_for(names))
    ]
    chunks = [
        pltpu.make_async_copy(
            tok.at[m * rows : (m + 1) * rows, :], tokv.at[m * rows : (m + 1) * rows, :], tsem.at[m]
        )
        for m in range(tsem.shape[0])
    ]
    for c in chunks[:1] + fetch[:4] + chunks[1:] + fetch[4:]:
        c.start()
    return fetch, chunks, rows


NAMES = (
    ("a_send", 0), ("b_send", 0), ("a_send", 1), ("b_send", 1),
    ("a_keep", 0), ("b_keep", 0), ("a_keep", 1), ("b_keep", 1),
)


def project_kernel(tok, gain, w, *refs):
    outs = refs[:16]
    tokv, wv, obuf, ssq, gainv, tsem, wsem, osem, gsem = refs[16:]
    early = pltpu.make_async_copy(gain, gainv, gsem)
    early.start()
    fetch, chunks, rows = load_all(NAMES, tok, w, tokv, wv, tsem, wsem)
    n, d = tokv.shape
    early.wait()
    g = gainv[...].astype(F32).reshape(1, -1)
    done = []

    def ship(k):
        c = pltpu.make_async_copy(obuf.at[k, 0 : outs[k].shape[0], :], outs[k], osem.at[k])
        c.start()
        done.append(c)

    for k in range(0, 16, 4):
        for m, c in enumerate(chunks):
            at = slice(m * rows, (m + 1) * rows)
            if k == 0:
                c.wait()
                x = tokv[at, :].astype(F32)
                tokv[at, :] = (x * g).astype(BF)
                sq = x * x
                part = sum(sq[:, i : i + HD] for i in range(0, d, HD))
                ssq[:, at] = nt(jnp.ones((8, HD), BF), part.astype(BF))
            if m == 0:
                for f in fetch[k : k + 4]:
                    f.wait()
            r = jnp.dot(tokv[at, :], wv[:, k * HD : (k + 4) * HD], preferred_element_type=F32).astype(BF)
            for i in range(4):
                if k < 8:
                    obuf[k + i, at, :] = r[:, i * HD : (i + 1) * HD]
                else:
                    outs[k + i][at, :] = r[:, i * HD : (i + 1) * HD]
        if k == 0:
            parts = [ssq[0:1, i * HD : (i + 1) * HD] for i in range(n // HD)]
            tile = jnp.concatenate(parts + [jnp.zeros((16 - n // HD, HD), F32)], axis=0).astype(BF)
            for i in range(4):
                obuf[i, n : n + 16, :] = tile
                outs[8 + i][n : n + 16, :] = tile
        if k < 8:
            for i in range(4):
                ship(k + i)
    for c in done:
        c.wait()


VM = 50 << 20


def projection(kernel, count, chunks, tokens, gain, weight, extra, shapes, scratch, outs, sems):
    n, d = tokens.shape
    hbm = pl.BlockSpec(memory_space=pltpu.HBM)
    vmem = pl.BlockSpec(memory_space=pltpu.VMEM)
    return pl.pallas_call(
        kernel,
        in_specs=[hbm, hbm, hbm] + [vmem for _ in extra],
        out_specs=outs,
        scratch_shapes=[pltpu.VMEM((n, d), BF), pltpu.VMEM((d, count * HD), BF)]
        + scratch
        + [pltpu.SemaphoreType.DMA((chunks,)), pltpu.SemaphoreType.DMA((count,))]
        + sems,
        out_shape=[
            pltpu.HBM(s, BF) if o.memory_space == pltpu.HBM else jax.ShapeDtypeStruct(s, BF)
            for s, o in zip(shapes, outs)
        ],
        compiler_params=pltpu.CompilerParams(vmem_limit_bytes=VM),
    )(tokens, gain, weight, *extra)


def pair_kernel(a0, a1, b0, b1, oa, ob):
    oa[...] = a0[...] + a1[...]
    ob[...] = b0[...] + b1[...]


def pair_sum(a0, a1, b0, b1):
    return pl.pallas_call(
        pair_kernel, out_shape=[jax.ShapeDtypeStruct(a0.shape, BF)] * 2, compiler_params=small()
    )(a0, a1, b0, b1)


def own_kernel(a0, a1, a2, b0, b1, b2, give, keep):
    first = (lax.axis_index("tp_0") == 0).astype(jnp.int32)
    a = (a0[...].astype(F32) + a1[...].astype(F32) + a2[...].astype(F32)).astype(BF)
    b = (b0[...].astype(F32) + b1[...].astype(F32) + b2[...].astype(F32)).astype(BF)

    @pl.when(first == 1)
    def _():
        give[...] = b
        keep[...] = a

    @pl.when(first == 0)
    def _():
        give[...] = a
        keep[...] = b


def own_sum(*parts):
    return pl.pallas_call(
        own_kernel,
        out_shape=[jax.ShapeDtypeStruct(parts[0].shape, BF)] * 2,
        compiler_params=small(8),
    )(*parts)


def split3(x):
    hi = x.astype(BF)
    left = x - hi.astype(F32)
    mid = left.astype(BF)
    low = (left - mid.astype(F32)).astype(BF)
    return hi, mid, low


def page_group(x, op):
    lane = lax.broadcasted_iota(jnp.int32, x.shape, 1)
    n = x.shape[1]
    for k in (1, 2, 4, 8):
        other = jnp.where((lane & k) == 0, pltpu.roll(x, n - k, 1), pltpu.roll(x, k, 1))
        x = op(x, other)
    return x


def prepare_kernel(qown, qother, dest, row, mine, qpage, psel, wide, tags):
    pages = dest.shape[1]
    n = wide.shape[1]
    per_owner = 8
    dest_f, row_f = dest[...].astype(F32), row[...].astype(F32)
    p0 = lax.broadcasted_iota(jnp.int32, (pages, pages), 0)
    p1 = lax.broadcasted_iota(jnp.int32, (pages, pages), 1)
    column = lambda v: jnp.sum(jnp.where(p0 == p1, v, 0.0), axis=1, keepdims=True)
    dest_c = column(dest_f)
    half = qown.shape[0]
    place = (dest[...] ^ mine[0]).astype(F32)
    where_page = column(place * per_owner + row_f)
    lanes = lax.broadcasted_iota(jnp.int32, (pages, half), 1).astype(F32)
    pick = lambda shift: (lanes + shift == where_page).astype(F32).astype(BF)
    qp = jnp.dot(pick(0.0), qown[...], preferred_element_type=F32) + jnp.dot(
        pick(float(half)), qother[...], preferred_element_type=F32
    )
    bp = PAGE
    for b in range(pages // bp):
        for j in range(8):
            at = (b * 8 + j) * bp
            qpage[at : at + bp, :] = qp[b * bp : (b + 1) * bp, j * HD : (j + 1) * HD].astype(BF)
    rank = jnp.sum(((dest_c == dest_f) & (p0 < p1)).astype(F32), axis=0, keepdims=True)
    place = (dest_f * SLOT + rank) * 2
    slots = psel.shape[1]
    at = lax.broadcasted_iota(jnp.int32, (slots, pages), 0).astype(F32)
    even = (at == place).astype(F32)
    odd = (at == place + 1).astype(F32)
    psel[0] = even.astype(BF)
    psel[1] = odd.astype(BF)
    token = lax.broadcasted_iota(jnp.int32, (pages, n), 1)
    page = lax.broadcasted_iota(jnp.int32, (pages, n), 0)
    head = (token == page * PAGE).astype(F32).astype(BF)
    wide[...] = jnp.dot((even + odd).astype(BF), head, preferred_element_type=F32).astype(BF)
    inside = (token // PAGE == page).astype(F32).astype(BF)
    tag8 = jnp.broadcast_to(row_f + 1.0, (8, pages)).astype(BF)
    tags[...] = jnp.dot(tag8, inside, preferred_element_type=F32)


def small(mib=6):
    return pltpu.CompilerParams(vmem_limit_bytes=mib << 20)


def prepare(qown, qother, dest, row, mine, slots, n):
    pages = dest.shape[1]
    return pl.pallas_call(
        prepare_kernel,
        out_shape=[
            jax.ShapeDtypeStruct((pages * 8, HD), BF),
            jax.ShapeDtypeStruct((2, slots * 2, pages), BF),
            jax.ShapeDtypeStruct((slots * 2, n), BF),
            jax.ShapeDtypeStruct((8, n), F32),
        ],
        in_specs=[pl.BlockSpec(memory_space=pltpu.VMEM)] * 4 + [pl.BlockSpec(memory_space=pltpu.SMEM)],
        compiler_params=small(),
        name="prepare",
    )(qown, qother, dest, row, mine)


def score_kernel(keys0, keys1, qpage, wide, tags, probs, ext, keys):
    n = keys0.shape[0] - 16
    ssum = keys0[n : n + 16, :].astype(F32) + keys1[n : n + 16, :].astype(F32)
    keys[...] = keys0[0:n, :] + keys1[0:n, :]
    block = 256
    bp = block // PAGE
    own = (
        lax.broadcasted_iota(jnp.int32, (bp, block), 1) // PAGE
        == lax.broadcasted_iota(jnp.int32, (bp, block), 0)
    )
    parts = []
    for b in range(n // block):
        q = qpage[b * 8 * bp : (b + 1) * 8 * bp, :]
        s = nt(q, keys[b * block : (b + 1) * block, :]).reshape(8, bp, block)
        parts.append(jnp.sum(jnp.where(own[None], s, 0.0), axis=1))
    total = jnp.concatenate([ssum[i : i + 1, :] for i in range(n // HD)], axis=1)
    scale = lax.rsqrt(total / 8192.0 + EPS)
    s = jnp.concatenate(parts, axis=1) * (scale * HD ** (-0.5))
    top = page_group(s, jnp.maximum)
    e = jnp.exp(s - top)
    mass = page_group(e, jnp.add)
    probs[...] = e / mass * scale
    hi, mid, low = split3(top + jnp.log(mass))
    stack = jnp.concatenate(
        [hi.astype(F32), mid.astype(F32), low.astype(F32), tags[...], jnp.zeros((HD - 32, n), F32)], axis=0
    ).astype(BF)
    ext[...] = nt(wide[...], stack).astype(BF)


def score(keys0, keys1, qpage, wide, tags):
    n = keys0.shape[0] - 16
    return pl.pallas_call(
        score_kernel,
        out_shape=[
            jax.ShapeDtypeStruct((8, n), F32),
            jax.ShapeDtypeStruct((wide.shape[0], HD), BF),
        ],
        scratch_shapes=[pltpu.VMEM((n, HD), BF)],
        compiler_params=small(),
        name="score",
    )(keys0, keys1, qpage, wide, tags)


def value_kernel(values0, values1, probs, ext, psel, out, acc):
    n = values0.shape[0]
    block = 256
    bp = block // PAGE
    own = (
        lax.broadcasted_iota(jnp.int32, (bp, block), 1) // PAGE
        == lax.broadcasted_iota(jnp.int32, (bp, block), 0)
    )
    for b in range(n // block):
        p = probs[:, b * block : (b + 1) * block]
        a = jnp.concatenate(
            [jnp.where(own, p[j : j + 1, :], 0.0) for j in range(8)], axis=0
        ).astype(BF)
        at = slice(b * block, (b + 1) * block)
        o = jnp.dot(a, values0[at, :] + values1[at, :], preferred_element_type=F32)
        for j in range(8):
            acc[b * bp : (b + 1) * bp, j * HD : (j + 1) * HD] = o[j * bp : (j + 1) * bp].astype(BF)
    half = acc.shape[1] // 2
    out[:, :half] = (
        jnp.dot(psel[0], acc[:, :half], preferred_element_type=F32)
        + jnp.dot(psel[1], acc[:, half:], preferred_element_type=F32)
    ).astype(BF)
    out[:, half:] = ext[...]


def value(values0, values1, probs, ext, psel):
    return pl.pallas_call(
        value_kernel,
        out_shape=jax.ShapeDtypeStruct((psel.shape[1], 5 * HD), BF),
        scratch_shapes=[pltpu.VMEM((psel.shape[2], 8 * HD), BF)],
        compiler_params=small(),
        name="value",
    )(values0, values1, probs, ext, psel)


def resident_kernel(queries, pool, table, length, fresh, top_out, mass_out, acc_out):
    rows = queries.shape[0]
    n = pool.shape[0]
    q32 = queries[...].astype(F32)
    q = jnp.concatenate([q32[:, j * HD : (j + 1) * HD] for j in range(8)], axis=0)
    s = nt(q.astype(BF), pool[:, :HD]) * HD ** (-0.5)
    token = lax.broadcasted_iota(jnp.int32, (rows, n), 1)
    valid = jnp.zeros((rows, n), jnp.int32)
    r0 = lax.broadcasted_iota(jnp.int32, (rows, rows), 0)
    r1 = lax.broadcasted_iota(jnp.int32, (rows, rows), 1)
    column = lambda v: jnp.sum(jnp.where(r0 == r1, v, 0), axis=1, keepdims=True)
    long = column(length[...])
    for i in range(table.shape[0]):
        hit = (token // PAGE == column(table[i : i + 1, :])) & (token % PAGE < long - PAGE * i)
        valid = valid + hit.astype(jnp.int32)
    mask = jnp.concatenate([valid] * 8, axis=0) > 0
    own = fresh[...].astype(F32)
    own_k = jnp.concatenate([own[:, :HD]] * 8, axis=0)
    own_v = jnp.concatenate([own[:, HD:]] * 8, axis=0)
    s_own = jnp.sum(q * own_k, axis=1, keepdims=True) * HD ** (-0.5)
    top = jnp.maximum(jnp.max(jnp.where(mask, s, -jnp.inf), axis=1, keepdims=True), s_own)
    e = jnp.where(mask, jnp.exp(s - top), 0.0)
    e_own = jnp.exp(s_own - top)
    top_out[...] = top
    mass_out[...] = jnp.sum(e, axis=1, keepdims=True) + e_own
    acc_out[...] = (
        jnp.dot(e.astype(BF), pool[:, HD:], preferred_element_type=F32) + e_own * own_v
    )


def resident(queries, pool, table, length, fresh):
    n = queries.shape[0] * 8
    return pl.pallas_call(
        resident_kernel,
        out_shape=[
            jax.ShapeDtypeStruct((n, 1), F32),
            jax.ShapeDtypeStruct((n, 1), F32),
            jax.ShapeDtypeStruct((n, HD), F32),
        ],
        compiler_params=small(),
        name="resident",
    )(queries, pool, table, length, fresh)


def merge_kernel(got, top_in, mass_in, acc_in, out):
    rows = out.shape[0]
    slots = got.shape[0]
    ext = got[:, 4 * HD :].astype(F32).T
    lse = ext[0:8] + ext[8:16] + ext[16:24]
    live = ext[24:25] == (lax.broadcasted_iota(jnp.int32, (rows, slots), 0) + 1).astype(F32)
    odd = lax.broadcasted_iota(jnp.int32, (rows, slots), 1) % 2
    for j in range(8):
        mask = live & (odd == j // 4)
        at = slice(j * rows, (j + 1) * rows)
        l = jnp.where(mask, lse[j : j + 1], -jnp.inf)
        top = jnp.maximum(jnp.max(l, axis=1, keepdims=True), top_in[at, :])
        w = jnp.where(mask, jnp.exp(l - top), 0.0)
        keep = jnp.exp(top_in[at, :] - top)
        total = jnp.sum(w, axis=1, keepdims=True) + mass_in[at, :] * keep
        k = j % 4
        o = jnp.dot(w.astype(BF), got[:, k * HD : (k + 1) * HD], preferred_element_type=F32)
        out[:, j * HD : (j + 1) * HD] = ((o + acc_in[at, :] * keep) / total).astype(BF)


def merge(got, top, mass, acc, rows):
    return pl.pallas_call(
        merge_kernel,
        out_shape=jax.ShapeDtypeStruct((rows, 8 * HD), BF),
        compiler_params=small(),
        name="merge",
    )(got, top, mass, acc)


def body(
    tokens,
    norm_gain,
    kv_weight,
    page_dest,
    page_row,
    queries,
    kv_pool,
    block_table,
    ctx_len,
    new_kv,
):
    n, d = tokens.shape
    ext, one = (n + 16, HD), (n, HD)
    gain = norm_gain

    vmem, hbm = pl.BlockSpec(memory_space=pltpu.VMEM), pl.BlockSpec(memory_space=pltpu.HBM)
    (
        kf_a, ko_a, kf_b, ko_b, vf_a, vo_a, vf_b, vo_b,
        kkf_a, kko_a, kkf_b, kko_b, vkf_a, vko_a, vkf_b, vko_b,
    ) = projection(
        project_kernel, 16, 2, tokens, gain, kv_weight, [],
        [ext] * 4 + [one] * 4 + [ext] * 4 + [one] * 4,
        [pltpu.VMEM((8, *ext), BF), pltpu.VMEM((8, n), F32), pltpu.VMEM((d,), BF)], [hbm] * 8 + [vmem] * 8,
        [pltpu.SemaphoreType.DMA((8,)), pltpu.SemaphoreType.DMA],
    )
    k1f_a, k1f_b = lax.ppermute(kf_a, "tp_1", NEAR), lax.ppermute(kf_b, "tp_1", FAR)
    k1o_a, k1o_b = lax.ppermute(ko_a, "tp_1", NEAR), lax.ppermute(ko_b, "tp_1", FAR)
    s_a, s_b = pair_sum(k1f_a, kkf_a, k1f_b, kkf_b)
    k2_a, k2_b = lax.ppermute(s_a, "tp_1", FAR), lax.ppermute(s_b, "tp_1", NEAR)
    v1f_a, v1f_b = lax.ppermute(vf_a, "tp_1", NEAR), lax.ppermute(vf_b, "tp_1", FAR)
    v1o_a, v1o_b = lax.ppermute(vo_a, "tp_1", NEAR), lax.ppermute(vo_b, "tp_1", FAR)
    owners = lax.axis_size(OWN)
    rows = queries.shape[0]
    peers = lax.axis_size("rep")
    spread = jnp.broadcast_to(queries[None], (peers, *queries.shape))
    qown = lax.all_to_all(spread, "rep", 0, 0, tiled=True).reshape(peers * rows, -1)
    qother = lax.ppermute(qown, "section", SWAP)
    s_a, s_b = pair_sum(v1f_a, vkf_a, v1f_b, vkf_b)
    v2_a, v2_b = lax.ppermute(s_a, "tp_1", FAR), lax.ppermute(s_b, "tp_1", NEAR)
    give, keep = own_sum(k1o_a, kko_a, k2_a, k1o_b, kko_b, k2_b)
    keys = (lax.ppermute(give, "tp_0", SWAP), keep)
    give, keep = own_sum(v1o_a, vko_a, v2_a, v1o_b, vko_b, v2_b)
    values = (lax.ppermute(give, "tp_0", SWAP), keep)

    pages = page_row.shape[0]
    mine = lax.axis_index("section").astype(jnp.int32).reshape(1) * peers
    qpage, psel, wide, tags = prepare(
        qown, qother, page_dest.reshape(1, pages), page_row.reshape(1, pages), mine,
        owners * SLOT, n,
    )
    top, mass, acc = resident(
        queries,
        kv_pool.reshape(-1, kv_pool.shape[2]),
        block_table.T,
        ctx_len.reshape(1, rows),
        new_kv,
    )
    probs, ext = score(*keys, qpage, wide, tags)
    sent = value(*values, probs, ext, psel)
    got = lax.all_to_all(sent.reshape(owners, 2 * SLOT, -1), OWN, 0, 0, tiled=True)
    return merge(got.reshape(owners * SLOT * 2, -1), top, mass, acc, rows)


def solution(mesh):
    split = Mesh(
        mesh.devices.reshape(mesh.shape["section"], mesh.shape["rep"], 2, 4),
        ("section", "rep", "tp_0", "tp_1"),
    )
    tp = ("tp_0", "tp_1")
    placed = (
        P(OWN, tp),
        P(tp),
        P(tp, None),
        P(OWN, None),
        P(OWN),
        P(OWN, tp),
        P(OWN, None, tp),
        P(OWN, None),
        P(OWN),
        P(OWN, tp),
    )

    return jax.shard_map(body, mesh=split, in_specs=placed, out_specs=P(OWN, tp), check_vma=False)
```
